512 devices in a mesh: dp: 4 (over x), seq: 16 (over z), feat: 8 (over y, core).
Axes of the slice: x: 4, y: 4, z: 16, core: 2. Of those that a mesh axis runs over, the one named last changes fastest.
Arguments:
- tokens: bfloat16 [65536, 2048], P(('dp', 'seq')), parts along dimension 0, may hold values from -6 to 6
- w_query: bfloat16 [2048, 256], P(None, 'feat'), may hold values from -0.125 to 0.125
- w_key: bfloat16 [2048, 256], P(None, 'feat'), may hold values from -0.125 to 0.125
- value_weight: bfloat16 [2048, 2048], P(None, 'feat'), may hold values from -0.125 to 0.125
- w_out: bfloat16 [2048, 2048], P(None, 'feat'), may hold values from -0.125 to 0.125
Outputs:
- mixed: bfloat16 [65536, 2048], P(('dp', 'seq'), 'feat'), parts along dimension 0
The draws below stay inside these ranges and needn't reach their ends.
There are 4 independent parts, one for each index of `dp`. The reference program is written for one: setup_inputs(seed, part) draws one part's arguments, and reference() takes and returns one part's arrays. A program takes and returns all parts, laid end to end along the dimension named above; an argument that names none is the same for every part. Nothing has to cross between parts.
All inputs are finite; a program needn't handle non-finite values.
Results may differ from the reference program's by a relative error of at most 0.009.
Values may be sent and summed in bfloat16 or wider, within the bound.
A program may use at most 64 MiB of HBM per device.

```python
import jax
import jax.numpy as jnp
from jax import lax

D = 2048
H = 16
DK = 16
DV = 128
TOK_DEV = 1024
SEQUENCE_TOKENS = 16384
N_SEQ = 16


def block_scale(rng, dims, shards, smallest, high):
    def one(dim, shards_of):
        heights = jax.random.uniform(jax.random.fold_in(jax.random.fold_in(rng, 6), dim), (shards_of,), jnp.float32, smallest / len(shards), high / len(shards))
        return jnp.repeat(jnp.exp(heights), dims[dim] // shards_of).reshape((-1,) + (1,) * (len(dims) - dim - 1))

    factor_of = one(*shards[0])
    for cut in shards[1:]:
        factor_of = factor_of * one(*cut)
    return factor_of


def bell_draw(rng, extent, deviation, most, shards=(), dtype=jnp.bfloat16):
    drawn = deviation * jax.random.normal(rng, extent, jnp.float32)
    if shards:
        drawn = drawn * block_scale(rng, extent, shards, -0.22, 0.18)
    return jnp.clip(drawn, -most, most).astype(dtype)


def setup_inputs(seed: int = 0, part: int = 0) -> dict:
    keys = jax.random.split(jax.random.key(seed), 6)
    own_keys = jax.random.split(jax.random.fold_in(keys[5], part), 6)
    tokens = bell_draw(own_keys[0], (SEQUENCE_TOKENS, D), 1.0, 6.0, ((0, 16),))
    w_query = bell_draw(keys[1], (D, H * DK), D ** -0.5, 0.125, ((1, 8),))
    w_key = bell_draw(keys[2], (D, H * DK), D ** -0.5, 0.125, ((1, 8),))
    value_weight = bell_draw(keys[3], (D, H * DV), D ** -0.5, 0.125, ((1, 8),))
    w_out = bell_draw(keys[4], (H * DV, D), (H * DV) ** -0.5, 0.125, ((1, 8),))
    return dict(tokens=tokens, w_query=w_query, w_key=w_key, value_weight=value_weight, w_out=w_out)


def key_features(key_rows):
    as_float = key_rows.astype(jnp.float32)
    row_count = key_rows.shape[0]
    head_total = key_rows.shape[1]
    linear = jnp.transpose(as_float, (1, 2, 0))
    square = jnp.einsum('nha,nhb->habn', as_float, as_float).reshape(head_total, -1, row_count)
    ones_row = jnp.ones((head_total, 1, row_count), jnp.float32)
    return jnp.concatenate([ones_row, linear, square], axis=1).astype(jnp.bfloat16)

def query_features(query_rows):
    as_float = query_rows.astype(jnp.float32)
    row_count = query_rows.shape[0]
    head_total = query_rows.shape[1]
    linear = jnp.transpose(as_float, (1, 2, 0)) * 0.25
    square = jnp.einsum('nha,nhb->habn', as_float, as_float).reshape(head_total, -1, row_count) * (1.0 / 32.0)
    ones_row = jnp.ones((head_total, 1, row_count), jnp.float32)
    return jnp.concatenate([ones_row, linear, square], axis=1)

def block_numerator(query_rows, key_rows, value_matrix, earlier):
    query_float = query_rows.astype(jnp.float32)
    key_float = key_rows.astype(jnp.float32)
    value_single = value_matrix.astype(jnp.float32)
    row_count = query_rows.shape[0]
    scores = jnp.einsum('nha,mha->hnm', query_float, key_float) * 0.25
    causal = lax.broadcasted_iota(jnp.int32, (row_count, row_count), 0) >= lax.broadcasted_iota(jnp.int32, (row_count, row_count), 1)
    weight_tensors = jnp.where(causal[None], 1.0 + scores + 0.5 * scores * scores, 0.0).astype(jnp.bfloat16)
    local_portion = jnp.einsum('iot,tiw->oiw', weight_tensors.astype(jnp.float32), value_single)
    carried = jnp.einsum('hfn,hfd->nhd', query_features(query_rows), earlier, precision=lax.Precision.HIGHEST)
    block_state = jnp.einsum('hfn,nhd->hfd', key_features(key_rows).astype(jnp.float32), value_single)
    return (carried + local_portion, block_state)

def reference(tokens, w_query, w_key, value_weight, w_out):
    query_all = jnp.dot(tokens, w_query, preferred_element_type=jnp.float32).astype(jnp.bfloat16).reshape(N_SEQ, TOK_DEV, H, DK)
    key_all = jnp.dot(tokens, w_key, preferred_element_type=jnp.float32).astype(jnp.bfloat16).reshape(N_SEQ, TOK_DEV, H, DK)
    value_all = jnp.dot(tokens, value_weight, preferred_element_type=jnp.float32).astype(jnp.bfloat16).reshape(N_SEQ, TOK_DEV, H, DV)

    def advance(prefix, items):
        numerator, block_state = block_numerator(items[0], items[1], items[2], prefix)
        return (prefix + block_state, numerator)
    initial = jnp.zeros((H, 1 + DK + DK * DK, DV), jnp.float32)
    final_state, numerator = lax.scan(advance, initial, (query_all, key_all, value_all))
    scale = lax.rsqrt(lax.optimization_barrier(jnp.mean(numerator * numerator, axis=-1, keepdims=True)) + 1e-06)
    normalized_rows = (numerator * scale).reshape(N_SEQ * TOK_DEV, H * DV).astype(jnp.bfloat16)
    return jnp.dot(normalized_rows, w_out, preferred_element_type=jnp.float32).astype(jnp.bfloat16)
```

```python
import functools

import jax
import jax.numpy as jnp
import numpy as np
from jax import lax
from jax.experimental import pallas as pl
from jax.experimental.pallas import tpu as pltpu
from jax.sharding import PartitionSpec as P

DK = 16
DV = 128
FEATS = 160
LANES = 128
ONE = 64
CHUNK = 16
CHUNKS = FEATS // CHUNK
MESH = pl.DeviceIdType.MESH


def selectors(first, ones_at, width, query):
    left = np.zeros((2 * FEATS, width), np.float32)
    right = np.zeros((2 * FEATS, width), np.float32)
    for head in range(2):
        row = head * FEATS
        base = first + head * DK
        left[row, ones_at] = 2.0 if query else 1.0
        right[row, ones_at] = 1.0
        row += 1
        for a in range(DK):
            left[row, base + a] = 0.5 if query else 1.0
            right[row, ones_at] = 1.0
            row += 1
        for a in range(DK):
            for b in range(a, DK):
                left[row, base + a] = (0.0625 if a == b else 0.125) if query else 1.0
                right[row, base + b] = 1.0
                row += 1
    return left, right


def remote(src, dst, send, recv, device):
    return pltpu.make_async_remote_copy(
        src_ref=src, dst_ref=dst, send_sem=send, recv_sem=recv, device_id=device, device_id_type=MESH
    )


def kernel(
    n_seq, tok, wq, wk, wv, wo, e1k, e2k, e1q, e2q, out,
    tok_v, wq_v, wk_v, wv_v, wqk_v, wo_v, e1k_v, e2k_v, e1q_v, e2q_v,
    qk_v, qkt, kaug, v_v, state, st, p1, p2, qx, phi, sx, lown, lx, acc_own, acc_oth, outp,
    load_sem, p1_send, p1_recv, p2_send, p2_recv, q_send, q_recv, w_send, w_recv,
    l_send, l_relay, l_recv, s_send, s_recv, o_send, o_recv,
):
    f32, bf16 = jnp.float32, jnp.bfloat16
    rows = tok.shape[0]
    rb = rows // 4
    half = rows // 2
    z = lax.axis_index("seq")
    f = lax.axis_index("feat")
    y = f // 2
    core = f % 2
    other = 1 - core
    yr, yl, yo = (y + 1) % 4, (y + 3) % 4, (y + 2) % 4
    partner = 2 * y + other

    barrier = pltpu.get_barrier_semaphore()
    for off in range(1, n_seq):
        pl.semaphore_signal(barrier, inc=1, device_id={"seq": (z + off) % n_seq}, device_id_type=MESH)
    for off in range(1, 8):
        pl.semaphore_signal(barrier, inc=1, device_id={"feat": (f + off) % 8}, device_id_type=MESH)

    def load(src, dst, k):
        return pltpu.make_async_copy(src, dst, load_sem.at[k])

    loads = [
        load(wq, wq_v, 0), load(wk, wk_v, 1), load(wv, wv_v, 2),
        *[load(tok.at[pl.ds(r * rb, rb)], tok_v.at[pl.ds(r * rb, rb)], 3 + r) for r in range(4)],
        load(e1k, e1k_v, 7), load(e2k, e2k_v, 8), load(e1q, e1q_v, 9), load(e2q, e2q_v, 10),
    ]
    own_w = load(wo, wo_v.at[core], 11)
    for copy in loads:
        copy.start()
    own_w.start()

    kaug[...] = jnp.zeros_like(kaug)
    one_row = (lax.broadcasted_iota(jnp.int32, (1, LANES), 1) == ONE).astype(f32)
    for k in range(8):
        qx[k, pl.ds(2 * DK, DK), :] = (
            lax.broadcasted_iota(jnp.int32, (DK, half), 0) == 0
        ).astype(f32).astype(bf16)
    loads[0].wait()
    loads[1].wait()
    wqk_v[...] = jnp.transpose(jnp.concatenate(
        [wq_v[...], wk_v[...], jnp.zeros((LANES - 4 * DK, wq_v.shape[1]), bf16)], axis=0
    ).astype(f32)).astype(bf16)
    loads[2].wait()
    for k in range(7, 11):
        if k == 7:
            loads[3].wait()
        loads[k].wait()

    for r in range(4):
        if r:
            loads[3 + r].wait()
        span = pl.ds(r * rb, rb)
        x = tok_v[span, :]
        qk = jnp.dot(x, wqk_v[...], preferred_element_type=f32) + one_row
        qk = qk.astype(bf16)
        qk_v[span, :] = qk
        turned = jnp.transpose(qk.astype(f32)).astype(bf16)
        qkt[:, span] = turned
        value = jnp.dot(x, wv_v[...], preferred_element_type=f32).astype(bf16)
        v_v[span, :] = value
        features = (
            jnp.dot(e1k_v[...], turned, preferred_element_type=f32)
            * jnp.dot(e2k_v[...], turned, preferred_element_type=f32)
        ).astype(bf16)
        for h in range(2):
            term = jnp.dot(
                features[h * FEATS:(h + 1) * FEATS], value[:, h * DV:(h + 1) * DV], preferred_element_type=f32
            )
            lanes = pl.ds(h * DV, DV)
            if r == 0:
                state[:, lanes] = term
            elif r < 3:
                state[:, lanes] += term
            else:
                st[:, lanes] = (state[:, lanes] + term).astype(bf16)

    pl.semaphore_wait(barrier, n_seq - 1 + 7)

    def owner_of(k):
        return (k * n_seq) // CHUNKS

    def chunk_of(device):
        k = (CHUNKS * device + n_seq - 1) // n_seq
        return jnp.minimum(k, CHUNKS - 1), (k < CHUNKS) & (owner_of(k) == device)

    my_chunk, is_owner = chunk_of(z)
    offsets = sorted(range(1, n_seq), key=lambda o: -min(o, n_seq - o))

    def to_owner(k, target):
        chunk, _ = chunk_of(target)
        return remote(
            st.at[pl.ds(pl.multiple_of(chunk * CHUNK, CHUNK), CHUNK)], p1.at[z],
            p1_send.at[k], p1_recv.at[z], {"seq": target},
        )

    for k, off in enumerate(offsets):
        target = (z + off) % n_seq

        @pl.when(chunk_of(target)[1])
        def _():
            to_owner(k, target).start()

    @pl.when(is_owner)
    def _():
        p1[z] = st[pl.ds(pl.multiple_of(my_chunk * CHUNK, CHUNK), CHUNK), :]

    q_copies = []
    for j in range(2):
        lanes = pl.ds(j * half, half)
        for k, yy in enumerate((yr, yl, yo)):
            q_copies.append(remote(
                qkt.at[pl.ds(0, 2 * DK), lanes], qx.at[f, pl.ds(0, 2 * DK)],
                q_send.at[j * 3 + k], q_recv.at[f], {"feat": 2 * yy + j},
            ))
    q_copies.append(remote(
        qkt.at[pl.ds(0, 2 * DK), pl.ds(pl.multiple_of(other * half, half), half)],
        qx.at[f, pl.ds(0, 2 * DK)], q_send.at[6], q_recv.at[f], {"feat": partner},
    ))
    for copy in q_copies:
        copy.start()
    qx[f, pl.ds(0, 2 * DK), :] = qkt[pl.ds(0, 2 * DK), pl.ds(pl.multiple_of(core * half, half), half)]

    own_w.wait()
    w_copy = remote(wo_v.at[core], wo_v.at[core], w_send, w_recv, {"feat": partner})
    w_copy.start()

    for h in range(2):
        kaug[h, pl.ds(h * DK, DK), :] = (
            qkt[pl.ds((2 + h) * DK, DK), :].astype(f32) * 0.25
        ).astype(bf16)
        kaug[h, pl.ds(ONE, DK), :] = qkt[pl.ds(ONE, DK), :]
    causal = lax.broadcasted_iota(jnp.int32, (rb, rb), 0) >= lax.broadcasted_iota(jnp.int32, (rb, rb), 1)
    l_copies = []
    for r in range(4):
        span = pl.ds(r * rb, rb)
        j, b = r // 2, r % 2
        for h in range(2):
            lanes = pl.ds(h * DV, DV)
            raised = jnp.dot(
                qk_v[span, :], kaug[h, :, pl.ds(r * rb, rb)], preferred_element_type=f32
            )
            weight = jnp.where(causal, raised * raised + 1.0, 0.0).astype(bf16)
            total = jnp.dot(weight, v_v[span, lanes], preferred_element_type=f32)
            if r:
                raised = jnp.dot(
                    qk_v[span, :], kaug[h, :, pl.ds(0, r * rb)], preferred_element_type=f32
                )
                weight = (raised * raised + 1.0).astype(bf16)
                total += jnp.dot(weight, v_v[pl.ds(0, r * rb), lanes], preferred_element_type=f32)
            lown[span, lanes] = total.astype(bf16)

        for k, yy in enumerate((yr, yl)):
            copy = remote(
                lown.at[span], lx.at[f, pl.ds(b * rb, rb)], l_send.at[r, k], l_recv.at[f, b],
                {"feat": 2 * yy + j},
            )
            copy.start()
            l_copies.append(copy)
        across = remote(
            lown.at[span], lx.at[f, pl.ds(b * rb, rb)], l_send.at[r, 2], l_recv.at[f, b],
            {"feat": partner},
        )

        @pl.when(core != j)
        def _():
            across.start()

        @pl.when(core == j)
        def _():
            lx[f, pl.ds(b * rb, rb), :] = lown[span, :]

    def make_phi(g, _):
        source = (f + g) % 8

        @pl.when(g > 0)
        def _():
            remote(
                qkt.at[pl.ds(0, 2 * DK), pl.ds(0, half)], qx.at[source, pl.ds(0, 2 * DK)],
                q_send.at[0], q_recv.at[source], {"feat": partner},
            ).wait_recv()

        q = qx[source]
        turned = (
            jnp.dot(e1q_v[...], q, preferred_element_type=f32)
            * jnp.dot(e2q_v[...], q, preferred_element_type=f32)
        )
        for h in range(2):
            phi[source, h] = jnp.transpose(turned[h * FEATS:(h + 1) * FEATS]).astype(bf16)
        return 0

    lax.fori_loop(0, 8, make_phi, 0)

    def back(k, target):
        return remote(
            p2.at[target], sx.at[f, pl.ds(pl.multiple_of(my_chunk * CHUNK, CHUNK), CHUNK)],
            p2_send.at[k], p2_recv.at[my_chunk], {"seq": target},
        )

    @pl.when(is_owner)
    def _():
        def arrive(s, _):
            @pl.when(s != z)
            def _():
                remote(
                    st.at[pl.ds(0, CHUNK)], p1.at[s], p1_send.at[0], p1_recv.at[s], {"seq": s}
                ).wait_recv()
            return 0

        lax.fori_loop(0, n_seq, arrive, 0)
        total = jnp.zeros((CHUNK, 2 * DV), f32)
        for c in range(n_seq):
            p2[c] = total.astype(bf16)
            total = total + p1[c].astype(f32)
        for k, off in enumerate(offsets):
            back(k, (z + off) % n_seq).start()
        sx[f, pl.ds(pl.multiple_of(my_chunk * CHUNK, CHUNK), CHUNK), :] = p2[z]

    def l_wait(source, b):
        remote(
            lown.at[pl.ds(0, rb)], lx.at[source, pl.ds(b * rb, rb)], l_send.at[0, 0],
            l_recv.at[source, b], {"feat": partner},
        ).wait_recv()

    relays = []
    for b in range(2):
        for k, (source, to) in enumerate(((2 * yl, yr), (2 * yr + 1, yl))):
            l_wait(source, b)
            copy = remote(
                lx.at[source, pl.ds(b * rb, rb)], lx.at[source, pl.ds(b * rb, rb)],
                l_relay.at[k, b], l_recv.at[source, b], {"feat": 2 * to + core},
            )
            copy.start()
            relays.append(copy)

    def chunk_in(k, _):
        @pl.when(owner_of(k) != z)
        def _():
            remote(
                p2.at[0], sx.at[f, pl.ds(pl.multiple_of(k * CHUNK, CHUNK), CHUNK)],
                p2_send.at[0], p2_recv.at[k], {"seq": 0},
            ).wait_recv()
        return 0

    lax.fori_loop(0, CHUNKS, chunk_in, 0)

    def s_copy(k, source, target):
        return remote(sx.at[source], sx.at[source], s_send.at[k], s_recv.at[source], {"feat": target})

    def s_wait(source):
        s_copy(0, source, partner).wait_recv()

    near = (2 * yr + core, 2 * yl + core, 2 * yo + core)
    s_copies = [s_copy(k, f, target) for k, target in enumerate((near[2], near[0], near[1], partner))]
    for copy in s_copies:
        copy.start()

    w_copy.wait_recv()

    def finish(source, first=False):
        for h in range(2):
            lanes = pl.ds(h * DV, DV)
            number = jnp.dot(
                phi[source, h], sx[source, :, lanes], preferred_element_type=f32
            ) + lx[source, :, lanes].astype(f32)
            scale = lax.rsqrt(jnp.mean(number * number, axis=-1, keepdims=True) + 4e-6)
            lown[pl.ds(0, half), lanes] = (number * scale).astype(bf16)
        normed = lown[pl.ds(0, half), :]
        deep = pl.ds(pl.multiple_of(source * 2 * DV, 2 * DV), 2 * DV)
        for acc, which in ((acc_oth, other), (acc_own, core)):
            term = jnp.dot(normed, wo_v[which, deep, :], preferred_element_type=f32)
            if first:
                acc[...] = term
            else:
                acc[...] += term

    for copy in l_copies:
        copy.wait_send()
    for r in range(4):
        @pl.when(core != r // 2)
        def _():
            remote(
                lown.at[pl.ds(r * rb, rb)], lx.at[f, pl.ds((r % 2) * rb, rb)], l_send.at[r, 2],
                l_recv.at[f, r % 2], {"feat": partner},
            ).wait_send()

    finish(f, first=True)
    s_wait(partner)
    for b in range(2):
        l_wait(partner, b)
    finish(partner)
    passed = []
    for k, source in enumerate(near):
        s_wait(source)
        copy = s_copy(4 + k, source, partner)
        copy.start()
        passed.append(copy)
    for k, yy in enumerate((yr, yl, yo)):
        source = 2 * yy + core
        for b in range(2):
            if k == 0:
                @pl.when(core == 0)
                def _():
                    l_wait(source, b)
            elif k == 1:
                @pl.when(core == 1)
                def _():
                    l_wait(source, b)
            else:
                l_wait(source, b)
        finish(source)
    for k, yy in enumerate((yr, yl, yo)):
        source = 2 * yy + other
        s_wait(source)
        for b in range(2):
            if k == 0:
                @pl.when(other == 0)
                def _():
                    l_wait(source, b)
            elif k == 1:
                @pl.when(other == 1)
                def _():
                    l_wait(source, b)
            else:
                l_wait(source, b)
        finish(source)

    mine = pl.ds(pl.multiple_of(core * half, half), half)
    outp[...] = acc_oth[...].astype(bf16)
    out_copy = remote(outp, out.at[mine], o_send, o_recv, {"feat": partner})
    out_copy.start()
    out[mine, :] = acc_own[...].astype(bf16)

    for k, off in enumerate(offsets):
        target = (z + off) % n_seq

        @pl.when(chunk_of(target)[1])
        def _():
            to_owner(k, target).wait_send()

    @pl.when(is_owner)
    def _():
        for k, off in enumerate(offsets):
            back(k, (z + off) % n_seq).wait_send()

    for copy in q_copies + [w_copy] + relays + s_copies + passed:
        copy.wait_send()
    out_copy.wait_send()
    remote(
        outp, out.at[pl.ds(pl.multiple_of(other * half, half), half)], o_send, o_recv, {"feat": partner}
    ).wait_recv()


def local(n_seq, consts, tokens, w_query, w_key, value_weight, w_out):
    rows, deep = tokens.shape
    cols = value_weight.shape[1]
    half = rows // 2
    f32, bf16 = jnp.float32, jnp.bfloat16
    dma = pltpu.SemaphoreType.DMA
    anywhere = pl.BlockSpec(memory_space=pl.ANY)
    vm = pltpu.VMEM
    width = w_query.shape[1]
    return pl.pallas_call(
        functools.partial(kernel, n_seq),
        out_shape=jax.ShapeDtypeStruct((rows, cols), bf16),
        in_specs=[anywhere] * 9,
        out_specs=pl.BlockSpec(memory_space=pltpu.VMEM),
        scratch_shapes=[
            vm((rows, deep), bf16), vm((width, deep), bf16), vm((width, deep), bf16),
            vm((deep, cols), bf16), vm((deep, LANES), bf16), vm((2, 8 * cols, cols), bf16),
            vm((2 * FEATS, LANES), bf16), vm((2 * FEATS, LANES), bf16),
            vm((2 * FEATS, 3 * DK), bf16), vm((2 * FEATS, 3 * DK), bf16),
            vm((rows, LANES), bf16), vm((LANES, rows), bf16), vm((2, LANES, rows), bf16),
            vm((rows, cols), bf16), vm((FEATS, cols), f32), vm((FEATS, cols), bf16),
            vm((n_seq, CHUNK, cols), bf16), vm((n_seq, CHUNK, cols), bf16),
            vm((8, 3 * DK, half), bf16), vm((8, 2, half, FEATS), bf16), vm((8, FEATS, cols), bf16),
            vm((rows, cols), bf16), vm((8, half, cols), bf16),
            vm((half, cols), f32), vm((half, cols), f32), vm((half, cols), bf16),
            dma((12,)), dma((n_seq,)), dma((n_seq,)), dma((n_seq,)), dma((CHUNKS,)),
            dma((7,)), dma((8,)), dma, dma,
            dma((4, 3)), dma((2, 2)), dma((8, 2)), dma((7,)), dma((8,)), dma, dma,
        ],
        compiler_params=pltpu.CompilerParams(
            collective_id=0, has_side_effects=True, vmem_limit_bytes=56 * 1024 * 1024
        ),
    )(tokens, w_query.T, w_key.T, value_weight, w_out, *consts)


def solution(mesh):
    consts = [
        jnp.asarray(e, jnp.bfloat16)
        for e in (*selectors(2 * DK, ONE, LANES, False), *selectors(0, 2 * DK, 3 * DK, True))
    ]
    placed = (P(("dp", "seq"), None),) + (P(None, "feat"),) * 4

    def run(*args):
        return jax.shard_map(
            functools.partial(local, mesh.shape["seq"], consts),
            mesh=mesh, in_specs=placed, out_specs=P(("dp", "seq"), "feat"), check_vma=False,
        )(*args)

    return run
```

```python
import functools

import jax
import jax.numpy as jnp
import numpy as np
from jax import lax
from jax.experimental import pallas as pl
from jax.experimental.pallas import tpu as pltpu
from jax.sharding import PartitionSpec as P

DK = 16
DV = 128
FEATS = 160
LANES = 128
ONE = 64
CHUNK = 16
CHUNKS = FEATS // CHUNK
LOW = 3
MESH = pl.DeviceIdType.MESH


def selectors(first, ones_at, width, query):
    left = np.zeros((2 * FEATS, width), np.float32)
    right = np.zeros((2 * FEATS, width), np.float32)
    for head in range(2):
        row = head * FEATS
        base = first + head * DK
        left[row, ones_at] = 2.0 if query else 1.0
        right[row, ones_at] = 1.0
        row += 1
        for a in range(DK):
            left[row, base + a] = 0.5 if query else 1.0
            right[row, ones_at] = 1.0
            row += 1
        for a in range(DK):
            for b in range(a, DK):
                left[row, base + a] = (0.0625 if a == b else 0.125) if query else 1.0
                right[row, base + b] = 1.0
                row += 1
    return left, right


def remote(src, dst, send, recv, device):
    return pltpu.make_async_remote_copy(
        src_ref=src, dst_ref=dst, send_sem=send, recv_sem=recv, device_id=device, device_id_type=MESH
    )


def kernel(
    n_seq, tok, wq, wk, wv, wo, e1k, e2k, e1q, e2q, out,
    tok_v, wq_v, wk_v, wv_v, wqk_v, wo_v, e1k_v, e2k_v, e1q_v, e2q_v,
    qk_v, qkt, kaug, v_v, state, st, p1, p2, qx, phi, sx, early, lown, lx, nrm, acc, outp,
    load_sem, p1_send, p1_recv, e_recv, p2_send, p2_recv, q_send, q_recv, w_send, w_recv,
    l_send, l_relay, l_recv, s_send, s_recv, o_send, o_recv,
):
    f32, bf16 = jnp.float32, jnp.bfloat16
    rows = tok.shape[0]
    rb = rows // 4
    half = rows // 2
    z = lax.axis_index("seq")
    f = lax.axis_index("feat")
    y = f // 2
    core = f % 2
    other = 1 - core
    yr, yl, yo = (y + 1) % 4, (y + 3) % 4, (y + 2) % 4
    partner = 2 * y + other

    def signal(sem, **device):
        pl.semaphore_signal(sem, inc=1, device_id=device, device_id_type=MESH)

    barrier = pltpu.get_barrier_semaphore()
    for off in range(1, 8):
        signal(barrier, feat=(f + off) % 8)
    first_owner = LOW + 1
    is_low = z <= LOW
    is_last_low = z == LOW
    owns = (z >= first_owner) & (z < first_owner + CHUNKS)
    for t in range(LOW + 1):
        @pl.when(is_low & (z != t))
        def _():
            signal(barrier, seq=t)

    @pl.when(owns)
    def _():
        signal(barrier, seq=LOW)

    for t in range(first_owner, n_seq):
        @pl.when((z > LOW) & (z != t))
        def _():
            signal(barrier, seq=t)

    greetings = 7 + jnp.where(is_low, LOW, n_seq - 2 - LOW) + jnp.where(is_last_low, CHUNKS, 0)

    def load(src, dst, k):
        return pltpu.make_async_copy(src, dst, load_sem.at[k])

    w_loads = [load(wq, wq_v, 0), load(wk, wk_v, 1)]
    v_load = load(wv, wv_v, 2)
    t_loads = [load(tok.at[pl.ds(r * rb, rb)], tok_v.at[pl.ds(r * rb, rb)], 3 + r) for r in range(4)]
    k_loads = [load(e1k, e1k_v, 7), load(e2k, e2k_v, 8)]
    q_loads = [load(e1q, e1q_v, 9), load(e2q, e2q_v, 10)]
    own_w = load(wo, wo_v.at[core], 11)
    for copy in (*w_loads, v_load, t_loads[0], *k_loads, *t_loads[1:], *q_loads, own_w):
        copy.start()

    kaug[...] = jnp.zeros_like(kaug)
    one_row = (lax.broadcasted_iota(jnp.int32, (1, LANES), 1) == ONE).astype(f32)
    for k in range(8):
        qx[k, pl.ds(2 * DK, DK), :] = (
            lax.broadcasted_iota(jnp.int32, (DK, half), 0) == 0
        ).astype(f32).astype(bf16)
    for copy in w_loads:
        copy.wait()
    wqk_v[...] = jnp.transpose(jnp.concatenate(
        [wq_v[...], wk_v[...], jnp.zeros((LANES - 4 * DK, wq_v.shape[1]), bf16)], axis=0
    ).astype(f32)).astype(bf16)
    v_load.wait()

    causal = lax.broadcasted_iota(jnp.int32, (rb, rb), 0) >= lax.broadcasted_iota(jnp.int32, (rb, rb), 1)

    def project(r):
        span = pl.ds(r * rb, rb)
        x = tok_v[span, :]
        qk = (jnp.dot(x, wqk_v[...], preferred_element_type=f32) + one_row).astype(bf16)
        qk_v[span, :] = qk
        turned = jnp.transpose(qk.astype(f32)).astype(bf16)
        qkt[:, span] = turned
        for h in range(2):
            kaug[h, pl.ds(h * DK, DK), span] = (
                turned[(2 + h) * DK:(3 + h) * DK].astype(f32) * 0.25
            ).astype(bf16)
            kaug[h, pl.ds(ONE, DK), span] = turned[ONE:ONE + DK]
        v_v[span, :] = jnp.dot(x, wv_v[...], preferred_element_type=f32).astype(bf16)

    def add_state(r):
        span = pl.ds(r * rb, rb)
        turned = qkt[:, span]
        features = (
            jnp.dot(e1k_v[...], turned, preferred_element_type=f32)
            * jnp.dot(e2k_v[...], turned, preferred_element_type=f32)
        ).astype(bf16)
        for h in range(2):
            lanes = pl.ds(h * DV, DV)
            term = jnp.dot(features[h * FEATS:(h + 1) * FEATS], v_v[span, lanes], preferred_element_type=f32)
            if r == 0:
                state[:, lanes] = term
            elif r < 3:
                state[:, lanes] += term
            else:
                st[:, lanes] = (state[:, lanes] + term).astype(bf16)

    def own_portion(r):
        span = pl.ds(r * rb, rb)
        for h in range(2):
            lanes = pl.ds(h * DV, DV)
            raised = jnp.dot(qk_v[span, :], kaug[h, :, span], preferred_element_type=f32)
            weight = jnp.where(causal, raised * raised + 1.0, 0.0).astype(bf16)
            total = jnp.dot(weight, v_v[span, lanes], preferred_element_type=f32)
            if r:
                raised = jnp.dot(qk_v[span, :], kaug[h, :, pl.ds(0, r * rb)], preferred_element_type=f32)
                weight = (raised * raised + 1.0).astype(bf16)
                total += jnp.dot(weight, v_v[pl.ds(0, r * rb), lanes], preferred_element_type=f32)
            lown[span, lanes] = total.astype(bf16)

    def across(r):
        return remote(
            lown.at[pl.ds(r * rb, rb)], lx.at[f, pl.ds((r % 2) * rb, rb)], l_send.at[r, 2],
            l_recv.at[f, r % 2], {"feat": partner},
        )

    l_copies = []

    def send_portion(r):
        j, b = r // 2, r % 2
        for k, yy in enumerate((yr, yl)):
            copy = remote(
                lown.at[pl.ds(r * rb, rb)], lx.at[f, pl.ds(b * rb, rb)], l_send.at[r, k], l_recv.at[f, b],
                {"feat": 2 * yy + j},
            )
            copy.start()
            l_copies.append(copy)

        @pl.when(core != j)
        def _():
            across(r).start()

        @pl.when(core == j)
        def _():
            lx[f, pl.ds(b * rb, rb), :] = lown[pl.ds(r * rb, rb), :]

    t_loads[0].wait()
    project(0)
    for copy in k_loads:
        copy.wait()
    t_loads[1].wait()
    project(1)
    own_portion(0)
    add_state(0)
    pl.semaphore_wait(barrier, greetings)
    send_portion(0)
    t_loads[2].wait()
    project(2)
    own_portion(1)
    add_state(1)
    send_portion(1)
    t_loads[3].wait()
    project(3)
    add_state(2)
    add_state(3)

    my_chunk = jnp.clip(z - first_owner, 0, CHUNKS - 1)
    my_rows = pl.ds(pl.multiple_of(my_chunk * CHUNK, CHUNK), CHUNK)

    def to_low(t):
        return remote(st, early.at[jnp.minimum(z, LOW - 1)], p1_send.at[t], e_recv.at[jnp.minimum(z, LOW - 1)], {"seq": t})

    for t in range(LOW, 0, -1):
        @pl.when(z < t)
        def _():
            to_low(t).start()

    def to_owner(k):
        return remote(
            st.at[pl.ds(k * CHUNK, CHUNK)], p1.at[z], p1_send.at[k], p1_recv.at[z], {"seq": first_owner + k}
        )

    def chunks_out():
        for k in range(CHUNKS):
            @pl.when((z != first_owner + k) & (z != n_seq - 1))
            def _():
                to_owner(k).start()

    def gather_low():
        total = jnp.zeros(st.shape, f32)
        for t in range(LOW):
            @pl.when(t < z)
            def _():
                remote(st, early.at[t], p1_send.at[0], e_recv.at[t], {"seq": t}).wait_recv()

            total = total + jnp.where(t < z, early[t].astype(f32), 0.0)
        sx[f] = total.astype(bf16)
        return total

    @pl.when(z > LOW)
    def _():
        chunks_out()

    @pl.when(owns)
    def _():
        p1[z] = st[my_rows, :]

    q_copies = []
    for j in range(2):
        lanes = pl.ds(j * half, half)
        for k, yy in enumerate((yr, yl, yo)):
            q_copies.append(remote(
                qkt.at[pl.ds(0, 2 * DK), lanes], qx.at[f, pl.ds(0, 2 * DK)],
                q_send.at[j * 3 + k], q_recv.at[f], {"feat": 2 * yy + j},
            ))
    q_copies.append(remote(
        qkt.at[pl.ds(0, 2 * DK), pl.ds(pl.multiple_of(other * half, half), half)],
        qx.at[f, pl.ds(0, 2 * DK)], q_send.at[6], q_recv.at[f], {"feat": partner},
    ))
    for copy in q_copies:
        copy.start()
    own_portion(2)
    send_portion(2)
    own_portion(3)
    send_portion(3)
    qx[f, pl.ds(0, 2 * DK), :] = qkt[pl.ds(0, 2 * DK), pl.ds(pl.multiple_of(core * half, half), half)]

    @pl.when(is_last_low)
    def _():
        st[...] = (gather_low() + st[...].astype(f32)).astype(bf16)
        chunks_out()

    for copy in q_loads:
        copy.wait()
    own_w.wait()
    w_copy = remote(wo_v.at[core], wo_v.at[core], w_send, w_recv, {"feat": partner})
    w_copy.start()

    def make_phi(source):
        q = qx[source]
        turned = (
            jnp.dot(e1q_v[...], q, preferred_element_type=f32)
            * jnp.dot(e2q_v[...], q, preferred_element_type=f32)
        )
        for h in range(2):
            phi[source, h] = jnp.transpose(turned[h * FEATS:(h + 1) * FEATS]).astype(bf16)

    make_phi(f)

    def back(c):
        return remote(p2.at[c], sx.at[f, my_rows], p2_send.at[c], p2_recv.at[my_chunk], {"seq": c})

    @pl.when(owns)
    def _():
        total = jnp.zeros((CHUNK, 2 * DV), f32)
        for c in range(first_owner, n_seq):
            @pl.when(z != c - 1)
            def _():
                remote(
                    st.at[pl.ds(0, CHUNK)], p1.at[c - 1], p1_send.at[0], p1_recv.at[c - 1], {"seq": c - 1}
                ).wait_recv()

            total = total + p1[c - 1].astype(f32)
            p2[c] = total.astype(bf16)

            @pl.when(z != c)
            def _():
                back(c).start()

        sx[f, my_rows, :] = p2[z]

    def l_wait(source, b):
        remote(
            lown.at[pl.ds(0, rb)], lx.at[source, pl.ds(b * rb, rb)], l_send.at[0, 0],
            l_recv.at[source, b], {"feat": partner},
        ).wait_recv()

    relays = []

    def relay(b):
        for k, (source, to) in enumerate(((2 * yl, yr), (2 * yr + 1, yl))):
            l_wait(source, b)
            copy = remote(
                lx.at[source, pl.ds(b * rb, rb)], lx.at[source, pl.ds(b * rb, rb)],
                l_relay.at[k, b], l_recv.at[source, b], {"feat": 2 * to + core},
            )
            copy.start()
            relays.append(copy)

    relay(0)

    def phi_of(g, _):
        source = (f + g) % 8
        remote(
            qkt.at[pl.ds(0, 2 * DK), pl.ds(0, half)], qx.at[source, pl.ds(0, 2 * DK)],
            q_send.at[0], q_recv.at[source], {"feat": partner},
        ).wait_recv()
        make_phi(source)
        return 0

    lax.fori_loop(1, 8, phi_of, 0)

    def chunk_in(k, _):
        @pl.when((z != first_owner + k) & (z > LOW))
        def _():
            remote(
                p2.at[0], sx.at[f, pl.ds(pl.multiple_of(k * CHUNK, CHUNK), CHUNK)],
                p2_send.at[0], p2_recv.at[k], {"feat": partner},
            ).wait_recv()
        return 0

    lax.fori_loop(0, CHUNKS, chunk_in, 0)

    @pl.when(z < LOW)
    def _():
        gather_low()

    def s_copy(k, source, target):
        return remote(sx.at[source], sx.at[source], s_send.at[k], s_recv.at[source], {"feat": target})

    def s_wait(source):
        s_copy(0, source, partner).wait_recv()

    near = (2 * yr + core, 2 * yl + core, 2 * yo + core)
    s_copies = [s_copy(k, f, target) for k, target in enumerate((near[2], near[0], near[1], partner))]
    for copy in s_copies:
        copy.start()
    relay(1)
    w_copy.wait_recv()

    def finish(units, first=False):
        for u, (source, b) in enumerate(units):
            span = pl.ds(b * rb, rb)
            for h in range(2):
                lanes = pl.ds(h * DV, DV)
                number = jnp.dot(
                    phi[source, h, span, :], sx[source, :, lanes], preferred_element_type=f32
                ) + lx[source, span, lanes].astype(f32)
                scale = lax.rsqrt(jnp.mean(number * number, axis=-1, keepdims=True) + 4e-6)
                nrm[u, :, lanes] = (number * scale).astype(bf16)
        for b in range(2):
            span = pl.ds(b * rb, rb)
            mine = [(u, source) for u, (source, bb) in enumerate(units) if bb == b]
            for k, which in enumerate((other, core)):
                if mine:
                    term = sum(
                        jnp.dot(
                            nrm[u], wo_v[which, pl.ds(pl.multiple_of(source * 2 * DV, 2 * DV), 2 * DV), :],
                            preferred_element_type=f32,
                        )
                        for u, source in mine
                    )
                    acc[k, span, :] = term if first else acc[k, span, :] + term

    def l_wait_unless_relayed(source, b):
        @pl.when((source != 2 * yl) & (source != 2 * yr + 1))
        def _():
            l_wait(source, b)

    finish([(f, 0), (f, 1)], first=True)
    s_wait(partner)
    for b in range(2):
        l_wait(partner, b)
    finish([(partner, 0), (partner, 1)])
    passed = []

    def s_pass(k):
        s_wait(near[k])
        copy = s_copy(4 + k, near[k], partner)
        copy.start()
        passed.append(copy)

    def sides(sources):
        units = [(source, b) for source in sources for b in range(2)]
        for source, b in units:
            l_wait_unless_relayed(source, b)
        finish(units)

    s_pass(0)
    s_pass(1)
    sides(near[:2])
    s_pass(2)
    beyond = (2 * yr + other, 2 * yl + other, 2 * yo + other)
    s_wait(beyond[0])
    s_wait(beyond[1])
    sides(beyond[:2])
    s_wait(beyond[2])
    out_copies = []
    for b in range(2):
        units = [(near[2], b), (beyond[2], b)]
        for source, _ in units:
            l_wait(source, b)
        finish(units)
        span = pl.ds(b * rb, rb)
        mine = pl.ds(pl.multiple_of(core * half + b * rb, rb), rb)
        outp[span, :] = acc[0, span, :].astype(bf16)
        out_copy = remote(outp.at[span], out.at[mine], o_send.at[b], o_recv.at[b], {"feat": partner})
        out_copy.start()
        out_copies.append(out_copy)
        out[mine, :] = acc[1, span, :].astype(bf16)

    for t in range(LOW, 0, -1):
        @pl.when(z < t)
        def _():
            to_low(t).wait_send()

    for k in range(CHUNKS):
        @pl.when((z >= LOW) & (z != first_owner + k) & (z != n_seq - 1))
        def _():
            to_owner(k).wait_send()

    @pl.when(owns)
    def _():
        for c in range(first_owner, n_seq):
            @pl.when(z != c)
            def _():
                back(c).wait_send()

    for r in range(4):
        @pl.when(core != r // 2)
        def _():
            across(r).wait_send()

    for copy in l_copies + q_copies + [w_copy] + relays + s_copies + passed + out_copies:
        copy.wait_send()
    for b in range(2):
        theirs = pl.ds(pl.multiple_of(other * half + b * rb, rb), rb)
        remote(
            outp.at[pl.ds(b * rb, rb)], out.at[theirs], o_send.at[b], o_recv.at[b], {"feat": partner}
        ).wait_recv()


def local(n_seq, consts, tokens, w_query, w_key, value_weight, w_out):
    rows, deep = tokens.shape
    cols = value_weight.shape[1]
    half = rows // 2
    f32, bf16 = jnp.float32, jnp.bfloat16
    dma = pltpu.SemaphoreType.DMA
    anywhere = pl.BlockSpec(memory_space=pl.ANY)
    vm = pltpu.VMEM
    width = w_query.shape[1]
    return pl.pallas_call(
        functools.partial(kernel, n_seq),
        out_shape=jax.ShapeDtypeStruct((rows, cols), bf16),
        in_specs=[anywhere] * 9,
        out_specs=pl.BlockSpec(memory_space=pltpu.VMEM),
        scratch_shapes=[
            vm((rows, deep), bf16), vm((width, deep), bf16), vm((width, deep), bf16),
            vm((deep, cols), bf16), vm((deep, LANES), bf16), vm((2, 8 * cols, cols), bf16),
            vm((2 * FEATS, LANES), bf16), vm((2 * FEATS, LANES), bf16),
            vm((2 * FEATS, 3 * DK), bf16), vm((2 * FEATS, 3 * DK), bf16),
            vm((rows, LANES), bf16), vm((LANES, rows), bf16), vm((2, LANES, rows), bf16),
            vm((rows, cols), bf16), vm((FEATS, cols), f32), vm((FEATS, cols), bf16),
            vm((n_seq, CHUNK, cols), bf16), vm((n_seq, CHUNK, cols), bf16),
            vm((8, 3 * DK, half), bf16), vm((8, 2, half, FEATS), bf16), vm((8, FEATS, cols), bf16), vm((LOW, FEATS, cols), bf16),
            vm((rows, cols), bf16), vm((8, half, cols), bf16),
            vm((4, half // 2, cols), bf16), vm((2, half, cols), f32), vm((half, cols), bf16),
            dma((12,)), dma((CHUNKS,)), dma((n_seq,)), dma((LOW,)), dma((n_seq,)), dma((CHUNKS,)),
            dma((7,)), dma((8,)), dma, dma,
            dma((4, 3)), dma((2, 2)), dma((8, 2)), dma((7,)), dma((8,)), dma((2,)), dma((2,)),
        ],
        compiler_params=pltpu.CompilerParams(
            collective_id=0, has_side_effects=True, vmem_limit_bytes=56 * 1024 * 1024
        ),
    )(tokens, w_query.T, w_key.T, value_weight, w_out, *consts)


def solution(mesh):
    consts = [
        jnp.asarray(e, jnp.bfloat16)
        for e in (*selectors(2 * DK, ONE, LANES, False), *selectors(0, 2 * DK, 3 * DK, True))
    ]
    placed = (P(("dp", "seq"), None),) + (P(None, "feat"),) * 4

    def run(*args):
        return jax.shard_map(
            functools.partial(local, mesh.shape["seq"], consts),
            mesh=mesh, in_specs=placed, out_specs=P(("dp", "seq"), "feat"), check_vma=False,
        )(*args)

    return run
```

```python
import functools

import jax
import jax.numpy as jnp
import numpy as np
from jax import lax
from jax.experimental import pallas as pl
from jax.experimental.pallas import tpu as pltpu
from jax.sharding import PartitionSpec as P

DK = 16
DV = 128
FEATS = 160
LANES = 128
ONE = 64
CHUNK = 32
CHUNKS = FEATS // CHUNK
CHAIN = 8
HEAD = 3
FIRST_OWNER = 9
MESH = pl.DeviceIdType.MESH


def selectors(first, ones_at, width, query):
    left = np.zeros((2 * FEATS, width), np.float32)
    right = np.zeros((2 * FEATS, width), np.float32)
    for head in range(2):
        row = head * FEATS
        base = first + head * DK
        left[row, ones_at] = 2.0 if query else 1.0
        right[row, ones_at] = 1.0
        row += 1
        for a in range(DK):
            left[row, base + a] = 0.5 if query else 1.0
            right[row, ones_at] = 1.0
            row += 1
        for a in range(DK):
            for b in range(a, DK):
                left[row, base + a] = (0.0625 if a == b else 0.125) if query else 1.0
                right[row, base + b] = 1.0
                row += 1
    return left, right


def remote(src, dst, send, recv, device):
    return pltpu.make_async_remote_copy(
        src_ref=src, dst_ref=dst, send_sem=send, recv_sem=recv, device_id=device, device_id_type=MESH
    )


def kernel(
    n_seq, tok, wq, wk, wv, wo, e1k, e2k, e1q, e2q, out,
    tok_v, wq_v, wk_v, wv_v, wqk_v, wo_v, e1k_v, e2k_v, e1q_v, e2q_v,
    qk_v, qkt, kaug, v_v, state, st, p1, p2, pair_in, c_in, c_out, qx, phi, sx, lown, lx, nrm, acc, outp,
    load_sem, ready_sem, p1_send, p1_recv, p2_send, p2_recv, pair_send, pair_recv, c_send, c_recv, e_recv, q_send, q_recv, w_send, w_recv,
    l_send, l_relay, l_recv, s_send, s_recv, o_send, o_recv,
):
    f32, bf16 = jnp.float32, jnp.bfloat16
    rows = tok.shape[0]
    rb = rows // 4
    half = rows // 2
    z = lax.axis_index("seq")
    f = lax.axis_index("feat")
    y = f // 2
    core = f % 2
    other = 1 - core
    yr, yl, yo = (y + 1) % 4, (y + 3) % 4, (y + 2) % 4
    partner = 2 * y + other

    def signal(sem, **device):
        pl.semaphore_signal(sem, inc=1, device_id=device, device_id_type=MESH)

    barrier = pltpu.get_barrier_semaphore()
    for off in range(1, 8):
        signal(barrier, feat=(f + off) % 8)
    odd = z % 2 == 1
    last = CHAIN - 1
    chained = z < CHAIN
    owns = (z >= FIRST_OWNER) & (z < FIRST_OWNER + CHUNKS)
    gives = (z >= HEAD) & (z < n_seq - 1)

    @pl.when(chained & (z >= 1))
    def _():
        signal(barrier, seq=z - 1)

    @pl.when(chained & odd & (z >= 3))
    def _():
        signal(barrier, seq=z - 2)

    for k in range(CHUNKS):
        @pl.when((z >= HEAD) & (z != FIRST_OWNER + k))
        def _():
            signal(barrier, seq=FIRST_OWNER + k)

    for t in range(CHAIN, n_seq):
        @pl.when(owns & (z != t) & (not FIRST_OWNER <= t < FIRST_OWNER + CHUNKS))
        def _():
            signal(barrier, seq=t)

    greetings = 7 + jnp.where(
        chained,
        (z < last).astype(jnp.int32) + (odd & (z < last - 1)).astype(jnp.int32),
        jnp.where(owns, n_seq - HEAD - 1, CHUNKS),
    )

    def load(src, dst, k):
        return pltpu.make_async_copy(src, dst, load_sem.at[k])

    w_loads = [load(wq, wq_v, 0), load(wk, wk_v, 1)]
    v_load = load(wv, wv_v, 2)
    t_loads = [load(tok.at[pl.ds(r * rb, rb)], tok_v.at[pl.ds(r * rb, rb)], 3 + r) for r in range(4)]
    k_loads = [load(e1k, e1k_v, 7), load(e2k, e2k_v, 8)]
    q_loads = [load(e1q, e1q_v, 9), load(e2q, e2q_v, 10)]
    own_w = load(wo, wo_v.at[core], 11)
    for copy in (*w_loads, v_load, t_loads[0], *k_loads, *t_loads[1:], *q_loads, own_w):
        copy.start()

    kaug[...] = jnp.zeros_like(kaug)
    one_row = (lax.broadcasted_iota(jnp.int32, (1, LANES), 1) == ONE).astype(f32)
    for k in range(8):
        qx[k, pl.ds(2 * DK, DK), :] = (
            lax.broadcasted_iota(jnp.int32, (DK, half), 0) == 0
        ).astype(f32).astype(bf16)
    for copy in w_loads:
        copy.wait()
    wqk_v[...] = jnp.transpose(jnp.concatenate(
        [wq_v[...], wk_v[...], jnp.zeros((LANES - 4 * DK, wq_v.shape[1]), bf16)], axis=0
    ).astype(f32)).astype(bf16)
    v_load.wait()

    causal = lax.broadcasted_iota(jnp.int32, (rb, rb), 0) >= lax.broadcasted_iota(jnp.int32, (rb, rb), 1)

    def project(r):
        span = pl.ds(r * rb, rb)
        x = tok_v[span, :]
        qk = (jnp.dot(x, wqk_v[...], preferred_element_type=f32) + one_row).astype(bf16)
        qk_v[span, :] = qk
        turned = jnp.transpose(qk.astype(f32)).astype(bf16)
        qkt[:, span] = turned
        for h in range(2):
            kaug[h, pl.ds(h * DK, DK), span] = (
                turned[(2 + h) * DK:(3 + h) * DK].astype(f32) * 0.25
            ).astype(bf16)
            kaug[h, pl.ds(ONE, DK), span] = turned[ONE:ONE + DK]
        v_v[span, :] = jnp.dot(x, wv_v[...], preferred_element_type=f32).astype(bf16)

    def add_state(r):
        span = pl.ds(r * rb, rb)
        turned = qkt[:, span]
        features = (
            jnp.dot(e1k_v[...], turned, preferred_element_type=f32)
            * jnp.dot(e2k_v[...], turned, preferred_element_type=f32)
        ).astype(bf16)
        for h in range(2):
            lanes = pl.ds(h * DV, DV)
            term = jnp.dot(features[h * FEATS:(h + 1) * FEATS], v_v[span, lanes], preferred_element_type=f32)
            if r == 0:
                state[:, lanes] = term
            elif r < 3:
                state[:, lanes] += term
            else:
                st[:, lanes] = (state[:, lanes] + term).astype(bf16)

    def own_portion(r):
        span = pl.ds(r * rb, rb)
        for h in range(2):
            lanes = pl.ds(h * DV, DV)
            raised = jnp.dot(qk_v[span, :], kaug[h, :, span], preferred_element_type=f32)
            weight = jnp.where(causal, raised * raised + 1.0, 0.0).astype(bf16)
            total = jnp.dot(weight, v_v[span, lanes], preferred_element_type=f32)
            if r:
                raised = jnp.dot(qk_v[span, :], kaug[h, :, pl.ds(0, r * rb)], preferred_element_type=f32)
                weight = (raised * raised + 1.0).astype(bf16)
                total += jnp.dot(weight, v_v[pl.ds(0, r * rb), lanes], preferred_element_type=f32)
            lown[span, lanes] = total.astype(bf16)

    def across(r):
        return remote(
            lown.at[pl.ds(r * rb, rb)], lx.at[f, pl.ds((r % 2) * rb, rb)], l_send.at[r, 2],
            l_recv.at[f, r % 2], {"feat": partner},
        )

    l_copies = []

    def send_portion(r):
        j, b = r // 2, r % 2
        for k, yy in enumerate((yr, yl)):
            copy = remote(
                lown.at[pl.ds(r * rb, rb)], lx.at[f, pl.ds(b * rb, rb)], l_send.at[r, k], l_recv.at[f, b],
                {"feat": 2 * yy + j},
            )
            copy.start()
            l_copies.append(copy)

        @pl.when(core != j)
        def _():
            across(r).start()

        @pl.when(core == j)
        def _():
            lx[f, pl.ds(b * rb, rb), :] = lown[pl.ds(r * rb, rb), :]

    t_loads[0].wait()
    project(0)
    for copy in k_loads:
        copy.wait()
    t_loads[1].wait()
    project(1)
    own_portion(0)
    add_state(0)
    pl.semaphore_wait(barrier, greetings)
    for t in range(HEAD, CHAIN):
        @pl.when(owns)
        def _():
            signal(ready_sem, seq=t)

    send_portion(0)
    t_loads[2].wait()
    project(2)
    add_state(1)
    t_loads[3].wait()
    project(3)

    def q_copy(n, j, source, target):
        return remote(
            qkt.at[pl.ds(0, 2 * DK), pl.ds(pl.multiple_of(j * half, half), half)], qx.at[source, pl.ds(0, 2 * DK)],
            q_send.at[n], q_recv.at[source], {"feat": target},
        )

    q_copies = [q_copy(2 * j + k, j, f, 2 * yy + j) for j in range(2) for k, yy in enumerate((yr, yl))]
    q_copies.append(q_copy(4, other, f, partner))
    for copy in q_copies:
        copy.start()
    add_state(2)
    add_state(3)

    my_chunk = jnp.clip(z - FIRST_OWNER, 0, CHUNKS - 1)
    my_rows = pl.ds(pl.multiple_of(my_chunk * CHUNK, CHUNK), CHUNK)

    def pair_copy():
        return remote(st, pair_in, pair_send, pair_recv, {"seq": z + 1})

    @pl.when(chained & jnp.logical_not(odd))
    def _():
        pair_copy().start()

    def to_owner(k):
        return remote(
            st.at[pl.ds(k * CHUNK, CHUNK)], p1.at[z], p1_send.at[k], p1_recv.at[z], {"seq": FIRST_OWNER + k}
        )

    def chunks_out():
        for k in range(CHUNKS):
            @pl.when(z != FIRST_OWNER + k)
            def _():
                to_owner(k).start()

    @pl.when(gives & jnp.logical_not(chained))
    def _():
        chunks_out()

    @pl.when(owns)
    def _():
        p1[z] = st[my_rows, :]

    own_portion(1)
    send_portion(1)
    own_portion(2)
    send_portion(2)
    own_portion(3)
    send_portion(3)
    qx[f, pl.ds(0, 2 * DK), :] = qkt[pl.ds(0, 2 * DK), pl.ds(pl.multiple_of(core * half, half), half)]

    for copy in q_loads:
        copy.wait()
    own_w.wait()
    w_copy = remote(wo_v.at[core], wo_v.at[core], w_send, w_recv, {"feat": partner})
    w_copy.start()

    def make_phi(source):
        q = qx[source]
        turned = (
            jnp.dot(e1q_v[...], q, preferred_element_type=f32)
            * jnp.dot(e2q_v[...], q, preferred_element_type=f32)
        )
        for h in range(2):
            phi[source, h] = jnp.transpose(turned[h * FEATS:(h + 1) * FEATS]).astype(bf16)

    make_phi(f)

    near = (2 * yr + core, 2 * yl + core, 2 * yo + core)
    beyond = (2 * yr + other, 2 * yl + other, 2 * yo + other)

    def piece(k):
        return pl.ds(pl.multiple_of(k * CHUNK, CHUNK), CHUNK)

    def s_piece(n, k, source, target):
        return remote(
            sx.at[source, piece(k)], sx.at[source, piece(k)], s_send.at[n, k], s_recv.at[source, k],
            {"feat": target},
        )

    def to_odd(k):
        return remote(c_out.at[piece(k)], c_in.at[piece(k)], c_send.at[0, k], c_recv.at[k], {"seq": z + 2})

    def to_even(k):
        return remote(c_out.at[piece(k)], sx.at[f, piece(k)], c_send.at[1, k], e_recv.at[k], {"seq": z + 1})

    def chain():
        @pl.when(z == 0)
        def _():
            sx[f] = jnp.zeros(sx.shape[1:], bf16)

        @pl.when(odd)
        def _():
            pair_copy().wait_recv()

        def step(k, _):
            @pl.when(odd)
            def _():
                @pl.when(z >= 3)
                def _():
                    to_odd(k).wait_recv()

                before = jnp.where(z >= 3, c_in[piece(k), :].astype(f32), 0.0) + pair_in[piece(k), :].astype(f32)
                c_out[piece(k), :] = (before + st[piece(k), :].astype(f32)).astype(bf16)
                sx[f, piece(k), :] = before.astype(bf16)

                @pl.when(z < last - 1)
                def _():
                    to_odd(k).start()

                @pl.when(z < last)
                def _():
                    to_even(k).start()

            @pl.when(jnp.logical_not(odd) & (z >= 2))
            def _():
                to_even(k).wait_recv()

            for n, target in enumerate((near[0], near[1], partner)):
                s_piece(n, k, f, target).start()
            return 0

        lax.fori_loop(0, CHUNKS, step, 0)

    @pl.when(chained)
    def _():
        @pl.when(z > HEAD)
        def _():
            pl.semaphore_wait(ready_sem, CHUNKS)
            chunks_out()

        chain()

        @pl.when(z == HEAD)
        def _():
            pl.semaphore_wait(ready_sem, CHUNKS)
            st[...] = c_out[...]
            chunks_out()

    def back(c):
        return remote(p2.at[c], sx.at[f, my_rows], p2_send.at[c], p2_recv.at[my_chunk], {"seq": c})

    def own_chunk():
        total = jnp.zeros((CHUNK, 2 * DV), f32)
        for c in range(HEAD + 1, n_seq):
            @pl.when(z != c - 1)
            def _():
                remote(
                    st.at[pl.ds(0, CHUNK)], p1.at[c - 1], p1_send.at[0], p1_recv.at[c - 1], {"seq": c - 1}
                ).wait_recv()

            total = total + p1[c - 1].astype(f32)
            if c >= CHAIN:
                p2[c] = total.astype(bf16)

                @pl.when(z != c)
                def _():
                    back(c).start()

        sx[f, my_rows, :] = p2[z]

    def from_owners():
        def step(k, _):
            @pl.when(z != FIRST_OWNER + k)
            def _():
                remote(
                    p2.at[0], sx.at[f, piece(k)], p2_send.at[0], p2_recv.at[k], {"feat": partner}
                ).wait_recv()

            for n, target in enumerate((near[0], near[1], partner)):
                s_piece(n, k, f, target).start()
            return 0

        lax.fori_loop(0, CHUNKS, step, 0)

    def l_wait(source, b):
        remote(
            lown.at[pl.ds(0, rb)], lx.at[source, pl.ds(b * rb, rb)], l_send.at[0, 0],
            l_recv.at[source, b], {"feat": partner},
        ).wait_recv()

    relays = []
    onward = ((2 * yl, yr), (2 * yr + 1, yl))
    for k, (source, to) in enumerate(onward):
        q_copy(0, 0, source, partner).wait_recv()
        copy = remote(
            qx.at[source, pl.ds(0, 2 * DK)], qx.at[source, pl.ds(0, 2 * DK)],
            q_send.at[5 + k], q_recv.at[source], {"feat": 2 * to + core},
        )
        copy.start()
        relays.append(copy)

    def l_onward(k, b):
        source, to = onward[k]
        span = pl.ds(b * rb, rb)
        return remote(
            lx.at[source, span], lx.at[source, span], l_relay.at[k, b], l_recv.at[source, b],
            {"feat": 2 * to + core},
        )

    def relay(b):
        for k, (source, to) in enumerate(onward):
            l_wait(source, b)
            l_onward(k, b).start()

    def phi_of(source):
        @pl.when((source != 2 * yl) & (source != 2 * yr + 1))
        def _():
            q_copy(0, 0, source, partner).wait_recv()

        make_phi(source)

    def phi_near(g, _):
        phi_of(jnp.where(g < 4, 2 * jnp.where(g < 2, yr, yl) + g % 2, partner))
        return 0

    def phi_far(g, _):
        phi_of(2 * yo + g)
        return 0

    lax.fori_loop(0, 5, phi_near, 0)

    @pl.when(owns)
    def _():
        own_chunk()

    relay(0)
    @pl.when(jnp.logical_not(chained))
    def _():
        from_owners()

    relay(1)

    def s_wait(source):
        for k in range(CHUNKS):
            s_piece(0, k, source, partner).wait_recv()

    def s_pass(n):
        for k in range(CHUNKS):
            s_piece(0, k, near[n], partner).wait_recv()
            if n < 2:
                @pl.when(core == 1 - n)
                def _():
                    s_piece(6, k, near[n], near[1 - n]).start()
            s_piece(3 + n, k, near[n], partner).start()

    lax.fori_loop(0, 2, phi_far, 0)
    w_copy.wait_recv()

    def finish(units, first=False):
        for u, (source, b) in enumerate(units):
            span = pl.ds(b * rb, rb)
            for h in range(2):
                lanes = pl.ds(h * DV, DV)
                number = jnp.dot(
                    phi[source, h, span, :], sx[source, :, lanes], preferred_element_type=f32
                ) + lx[source, span, lanes].astype(f32)
                scale = lax.rsqrt(jnp.mean(number * number, axis=-1, keepdims=True) + 4e-6)
                nrm[u, :, lanes] = (number * scale).astype(bf16)
        for b in range(2):
            span = pl.ds(b * rb, rb)
            mine = [(u, source) for u, (source, bb) in enumerate(units) if bb == b]
            for k, which in enumerate((other, core)):
                if mine:
                    term = sum(
                        jnp.dot(
                            nrm[u], wo_v[which, pl.ds(pl.multiple_of(source * 2 * DV, 2 * DV), 2 * DV), :],
                            preferred_element_type=f32,
                        )
                        for u, source in mine
                    )
                    acc[k, span, :] = term if first else acc[k, span, :] + term

    def l_wait_unless_relayed(source, b):
        @pl.when((source != 2 * yl) & (source != 2 * yr + 1))
        def _():
            l_wait(source, b)

    finish([(f, 0), (f, 1)], first=True)
    s_wait(partner)
    for b in range(2):
        l_wait(partner, b)
    finish([(partner, 0), (partner, 1)])
    def sides(sources):
        units = [(source, b) for source in sources for b in range(2)]
        for source, b in units:
            l_wait_unless_relayed(source, b)
        finish(units)

    s_pass(0)
    s_pass(1)
    sides(near[:2])
    s_pass(2)
    s_wait(beyond[0])
    s_wait(beyond[1])
    sides(beyond[:2])
    s_wait(beyond[2])
    out_copies = []
    for b in range(2):
        units = [(near[2], b), (beyond[2], b)]
        for source, _ in units:
            l_wait(source, b)
        finish(units)
        span = pl.ds(b * rb, rb)
        mine = pl.ds(pl.multiple_of(core * half + b * rb, rb), rb)
        outp[span, :] = acc[0, span, :].astype(bf16)
        out_copy = remote(outp.at[span], out.at[mine], o_send.at[b], o_recv.at[b], {"feat": partner})
        out_copy.start()
        out_copies.append(out_copy)
        out[mine, :] = acc[1, span, :].astype(bf16)

    with jax.named_scope('tail_sends'):
        @pl.when(chained & jnp.logical_not(odd))
        def _():
            pair_copy().wait_send()

        for k in range(CHUNKS):
            @pl.when(chained & odd & (z < last - 1))
            def _():
                to_odd(k).wait_send()

            @pl.when(chained & odd & (z < last))
            def _():
                to_even(k).wait_send()

            @pl.when(gives & (z != FIRST_OWNER + k))
            def _():
                to_owner(k).wait_send()

        @pl.when(owns)
        def _():
            for c in range(CHAIN, n_seq):
                @pl.when(z != c)
                def _():
                    back(c).wait_send()

        for r in range(4):
            @pl.when(core != r // 2)
            def _():
                across(r).wait_send()

        for copy in l_copies + q_copies + [w_copy] + relays + out_copies:
            copy.wait_send()
        for k in range(2):
            for b in range(2):
                l_onward(k, b).wait_send()
        for n, source in enumerate((f, f, f, near[0], near[1], near[2], f)):
            for k in range(CHUNKS):
                s_piece(n, k, source, partner).wait_send()
    with jax.named_scope('tail_recv'):
        for b in range(2):
            theirs = pl.ds(pl.multiple_of(other * half + b * rb, rb), rb)
            remote(
                outp.at[pl.ds(b * rb, rb)], out.at[theirs], o_send.at[b], o_recv.at[b], {"feat": partner}
            ).wait_recv()


def local(n_seq, consts, tokens, w_query, w_key, value_weight, w_out):
    rows, deep = tokens.shape
    cols = value_weight.shape[1]
    half = rows // 2
    f32, bf16 = jnp.float32, jnp.bfloat16
    dma = pltpu.SemaphoreType.DMA
    anywhere = pl.BlockSpec(memory_space=pl.ANY)
    vm = pltpu.VMEM
    width = w_query.shape[1]
    mixed = pl.pallas_call(
        functools.partial(kernel, n_seq),
        out_shape=pltpu.VMEM((rows, cols), bf16),
        in_specs=[anywhere] * 9,
        out_specs=pl.BlockSpec(memory_space=pltpu.VMEM),
        scratch_shapes=[
            vm((rows, deep), bf16), vm((width, deep), bf16), vm((width, deep), bf16),
            vm((deep, cols), bf16), vm((deep, LANES), bf16), vm((2, 8 * cols, cols), bf16),
            vm((2 * FEATS, LANES), bf16), vm((2 * FEATS, LANES), bf16),
            vm((2 * FEATS, 3 * DK), bf16), vm((2 * FEATS, 3 * DK), bf16),
            vm((rows, LANES), bf16), vm((LANES, rows), bf16), vm((2, LANES, rows), bf16),
            vm((rows, cols), bf16), vm((FEATS, cols), f32), vm((FEATS, cols), bf16),
            vm((n_seq, CHUNK, cols), bf16), vm((n_seq, CHUNK, cols), bf16),
            vm((FEATS, cols), bf16), vm((FEATS, cols), bf16), vm((FEATS, cols), bf16),
            vm((8, 3 * DK, half), bf16), vm((8, 2, half, FEATS), bf16), vm((8, FEATS, cols), bf16),
            vm((rows, cols), bf16), vm((8, half, cols), bf16),
            vm((4, half // 2, cols), bf16), vm((2, half, cols), f32), vm((half, cols), bf16),
            dma((12,)), pltpu.SemaphoreType.REGULAR,
            dma((CHUNKS,)), dma((n_seq,)), dma((n_seq,)), dma((CHUNKS,)), dma, dma, dma((2, CHUNKS)), dma((CHUNKS,)), dma((CHUNKS,)),
            dma((7,)), dma((8,)), dma, dma,
            dma((4, 3)), dma((2, 2)), dma((8, 2)), dma((7, CHUNKS)), dma((8, CHUNKS)), dma((2,)), dma((2,)),
        ],
        compiler_params=pltpu.CompilerParams(
            collective_id=0, has_side_effects=True, vmem_limit_bytes=56 * 1024 * 1024
        ),
    )(tokens, w_query.T, w_key.T, value_weight, w_out, *consts)
    return mixed


def solution(mesh):
    consts = [
        jnp.asarray(e, jnp.bfloat16)
        for e in (*selectors(2 * DK, ONE, LANES, False), *selectors(0, 2 * DK, 3 * DK, True))
    ]
    placed = (P(("dp", "seq"), None),) + (P(None, "feat"),) * 4

    def run(*args):
        return jax.shard_map(
            functools.partial(local, mesh.shape["seq"], consts),
            mesh=mesh, in_specs=placed, out_specs=P(("dp", "seq"), "feat"), check_vma=False,
        )(*args)

    return run
```

```python
import functools

import jax
import jax.numpy as jnp
import numpy as np
from jax import lax
from jax.experimental import pallas as pl
from jax.experimental.pallas import tpu as pltpu
from jax.sharding import PartitionSpec as P

DK = 16
DV = 128
FEATS = 160
LANES = 128
ONE = 64
CHUNK = 32
CHUNKS = FEATS // CHUNK
CHAIN = 8
HEAD = 3
FIRST_OWNER = 10
MESH = pl.DeviceIdType.MESH


def selectors(first, ones_at, width, query):
    left = np.zeros((2 * FEATS, width), np.float32)
    right = np.zeros((2 * FEATS, width), np.float32)
    for head in range(2):
        row = head * FEATS
        base = first + head * DK
        left[row, ones_at] = 2.0 if query else 1.0
        right[row, ones_at] = 1.0
        row += 1
        for a in range(DK):
            left[row, base + a] = 0.5 if query else 1.0
            right[row, ones_at] = 1.0
            row += 1
        for a in range(DK):
            for b in range(a, DK):
                left[row, base + a] = (0.0625 if a == b else 0.125) if query else 1.0
                right[row, base + b] = 1.0
                row += 1
    return left, right


def remote(src, dst, send, recv, device):
    return pltpu.make_async_remote_copy(
        src_ref=src, dst_ref=dst, send_sem=send, recv_sem=recv, device_id=device, device_id_type=MESH
    )


def kernel(
    n_seq, tok, wq, wk, wv, wo, e1k, e2k, e1q, e2q, out,
    tok_v, wq_v, wk_v, wv_v, wqk_v, wo_v, e1k_v, e2k_v, e1q_v, e2q_v,
    qk_v, qkt, kaug, v_v, state, st, p1, p2, pair_in, c_in, c_out, qx, phi, sx, lown, lx, nrm, acc, outp,
    load_sem, ready_sem, p1_send, p1_recv, p2_send, p2_recv, pair_send, pair_recv, c_send, c_recv, e_recv, q_send, q_recv, w_send, w_recv,
    l_send, l_relay, l_recv, s_send, s_recv, o_send, o_recv,
):
    f32, bf16 = jnp.float32, jnp.bfloat16
    rows = tok.shape[0]
    rb = rows // 4
    half = rows // 2
    z = lax.axis_index("seq")
    f = lax.axis_index("feat")
    y = f // 2
    core = f % 2
    other = 1 - core
    yr, yl, yo = (y + 1) % 4, (y + 3) % 4, (y + 2) % 4
    partner = 2 * y + other

    def signal(sem, **device):
        pl.semaphore_signal(sem, inc=1, device_id=device, device_id_type=MESH)

    barrier = pltpu.get_barrier_semaphore()
    for off in range(1, 8):
        signal(barrier, feat=(f + off) % 8)
    odd = z % 2 == 1
    last = CHAIN - 1
    chained = z < CHAIN
    owns = (z >= FIRST_OWNER) & (z < FIRST_OWNER + CHUNKS)
    gives = (z >= HEAD) & (z < n_seq - 1)

    @pl.when(chained & (z >= 1))
    def _():
        signal(barrier, seq=z - 1)

    @pl.when(chained & odd & (z >= 3))
    def _():
        signal(barrier, seq=z - 2)

    for k in range(CHUNKS):
        @pl.when((z >= HEAD) & (z != FIRST_OWNER + k))
        def _():
            signal(barrier, seq=FIRST_OWNER + k)

    for t in range(CHAIN, n_seq):
        @pl.when(owns & (z != t) & (not FIRST_OWNER <= t < FIRST_OWNER + CHUNKS))
        def _():
            signal(barrier, seq=t)

    greetings = 7 + jnp.where(
        chained,
        (z < last).astype(jnp.int32) + (odd & (z < last - 1)).astype(jnp.int32),
        jnp.where(owns, n_seq - HEAD - 1, CHUNKS),
    )

    def load(src, dst, k):
        return pltpu.make_async_copy(src, dst, load_sem.at[k])

    w_loads = [load(wq, wq_v, 0), load(wk, wk_v, 1)]
    v_load = load(wv, wv_v, 2)
    t_loads = [load(tok.at[pl.ds(r * rb, rb)], tok_v.at[pl.ds(r * rb, rb)], 3 + r) for r in range(4)]
    k_loads = [load(e1k, e1k_v, 7), load(e2k, e2k_v, 8)]
    q_loads = [load(e1q, e1q_v, 9), load(e2q, e2q_v, 10)]
    own_w = load(wo, wo_v.at[core], 11)
    for copy in (*w_loads, v_load, t_loads[0], *k_loads, *t_loads[1:], *q_loads, own_w):
        copy.start()

    kaug[...] = jnp.zeros_like(kaug)
    one_row = (lax.broadcasted_iota(jnp.int32, (1, LANES), 1) == ONE).astype(f32)
    for k in range(8):
        qx[k, pl.ds(2 * DK, DK), :] = (
            lax.broadcasted_iota(jnp.int32, (DK, half), 0) == 0
        ).astype(f32).astype(bf16)
    for copy in w_loads:
        copy.wait()
    wqk_v[...] = jnp.transpose(jnp.concatenate(
        [wq_v[...], wk_v[...], jnp.zeros((LANES - 4 * DK, wq_v.shape[1]), bf16)], axis=0
    ).astype(f32)).astype(bf16)
    v_load.wait()

    causal = lax.broadcasted_iota(jnp.int32, (rb, rb), 0) >= lax.broadcasted_iota(jnp.int32, (rb, rb), 1)

    def project(r):
        span = pl.ds(r * rb, rb)
        x = tok_v[span, :]
        qk = (jnp.dot(x, wqk_v[...], preferred_element_type=f32) + one_row).astype(bf16)
        qk_v[span, :] = qk
        turned = jnp.transpose(qk.astype(f32)).astype(bf16)
        qkt[:, span] = turned
        for h in range(2):
            kaug[h, pl.ds(h * DK, DK), span] = (
                turned[(2 + h) * DK:(3 + h) * DK].astype(f32) * 0.25
            ).astype(bf16)
            kaug[h, pl.ds(ONE, DK), span] = turned[ONE:ONE + DK]
        v_v[span, :] = jnp.dot(x, wv_v[...], preferred_element_type=f32).astype(bf16)

    def add_state(r):
        span = pl.ds(r * rb, rb)
        turned = qkt[:, span]
        features = (
            jnp.dot(e1k_v[...], turned, preferred_element_type=f32)
            * jnp.dot(e2k_v[...], turned, preferred_element_type=f32)
        ).astype(bf16)
        for h in range(2):
            lanes = pl.ds(h * DV, DV)
            term = jnp.dot(features[h * FEATS:(h + 1) * FEATS], v_v[span, lanes], preferred_element_type=f32)
            if r == 0:
                state[:, lanes] = term
            elif r < 3:
                state[:, lanes] += term
            else:
                st[:, lanes] = (state[:, lanes] + term).astype(bf16)

    def own_portion(r):
        span = pl.ds(r * rb, rb)
        for h in range(2):
            lanes = pl.ds(h * DV, DV)
            raised = jnp.dot(qk_v[span, :], kaug[h, :, span], preferred_element_type=f32)
            weight = jnp.where(causal, raised * raised + 1.0, 0.0).astype(bf16)
            total = jnp.dot(weight, v_v[span, lanes], preferred_element_type=f32)
            if r:
                raised = jnp.dot(qk_v[span, :], kaug[h, :, pl.ds(0, r * rb)], preferred_element_type=f32)
                weight = (raised * raised + 1.0).astype(bf16)
                total += jnp.dot(weight, v_v[pl.ds(0, r * rb), lanes], preferred_element_type=f32)
            lown[span, lanes] = total.astype(bf16)

    def across(r):
        return remote(
            lown.at[pl.ds(r * rb, rb)], lx.at[f, pl.ds((r % 2) * rb, rb)], l_send.at[r, 2],
            l_recv.at[f, r % 2], {"feat": partner},
        )

    l_copies = []

    def send_portion(r):
        j, b = r // 2, r % 2
        for k, yy in enumerate((yr, yl)):
            copy = remote(
                lown.at[pl.ds(r * rb, rb)], lx.at[f, pl.ds(b * rb, rb)], l_send.at[r, k], l_recv.at[f, b],
                {"feat": 2 * yy + j},
            )
            copy.start()
            l_copies.append(copy)

        @pl.when(core != j)
        def _():
            across(r).start()

        @pl.when(core == j)
        def _():
            lx[f, pl.ds(b * rb, rb), :] = lown[pl.ds(r * rb, rb), :]

    t_loads[0].wait()
    project(0)
    for copy in k_loads:
        copy.wait()
    t_loads[1].wait()
    project(1)
    own_portion(0)
    add_state(0)
    pl.semaphore_wait(barrier, greetings)
    for t in range(HEAD, CHAIN):
        @pl.when(owns)
        def _():
            signal(ready_sem, seq=t)

    send_portion(0)
    t_loads[2].wait()
    project(2)
    add_state(1)
    t_loads[3].wait()
    project(3)

    def q_copy(n, j, source, target):
        return remote(
            qkt.at[pl.ds(0, 2 * DK), pl.ds(pl.multiple_of(j * half, half), half)], qx.at[source, pl.ds(0, 2 * DK)],
            q_send.at[n], q_recv.at[source], {"feat": target},
        )

    q_copies = [q_copy(2 * j + k, j, f, 2 * yy + j) for j in range(2) for k, yy in enumerate((yr, yl))]
    q_copies.append(q_copy(4, other, f, partner))
    for copy in q_copies:
        copy.start()
    add_state(2)
    add_state(3)

    my_chunk = jnp.clip(z - FIRST_OWNER, 0, CHUNKS - 1)
    my_rows = pl.ds(pl.multiple_of(my_chunk * CHUNK, CHUNK), CHUNK)

    def pair_copy():
        return remote(st, pair_in, pair_send, pair_recv, {"seq": z + 1})

    @pl.when(chained & jnp.logical_not(odd))
    def _():
        pair_copy().start()

    def to_owner(k):
        return remote(
            st.at[pl.ds(k * CHUNK, CHUNK)], p1.at[z], p1_send.at[k], p1_recv.at[z], {"seq": FIRST_OWNER + k}
        )

    def chunks_out():
        for k in range(CHUNKS):
            @pl.when(z != FIRST_OWNER + k)
            def _():
                to_owner(k).start()

    @pl.when(gives & jnp.logical_not(chained))
    def _():
        chunks_out()

    @pl.when(owns)
    def _():
        p1[z] = st[my_rows, :]

    own_portion(1)
    send_portion(1)
    own_portion(2)
    send_portion(2)
    own_portion(3)
    send_portion(3)
    qx[f, pl.ds(0, 2 * DK), :] = qkt[pl.ds(0, 2 * DK), pl.ds(pl.multiple_of(core * half, half), half)]

    for copy in q_loads:
        copy.wait()
    own_w.wait()
    w_copy = remote(wo_v.at[core], wo_v.at[core], w_send, w_recv, {"feat": partner})
    w_copy.start()

    def make_phi(source):
        q = qx[source]
        turned = (
            jnp.dot(e1q_v[...], q, preferred_element_type=f32)
            * jnp.dot(e2q_v[...], q, preferred_element_type=f32)
        )
        for h in range(2):
            phi[source, h] = jnp.transpose(turned[h * FEATS:(h + 1) * FEATS]).astype(bf16)

    make_phi(f)

    near = (2 * yr + core, 2 * yl + core, 2 * yo + core)
    beyond = (2 * yr + other, 2 * yl + other, 2 * yo + other)

    def piece(k):
        return pl.ds(pl.multiple_of(k * CHUNK, CHUNK), CHUNK)

    def s_piece(n, k, source, target):
        return remote(
            sx.at[source, piece(k)], sx.at[source, piece(k)], s_send.at[n, k], s_recv.at[source, k],
            {"feat": target},
        )

    def to_odd(k):
        return remote(c_out.at[piece(k)], c_in.at[piece(k)], c_send.at[0, k], c_recv.at[k], {"seq": z + 2})

    def to_even(k):
        return remote(c_out.at[piece(k)], sx.at[f, piece(k)], c_send.at[1, k], e_recv.at[k], {"seq": z + 1})

    def chain():
        @pl.when(z == 0)
        def _():
            sx[f] = jnp.zeros(sx.shape[1:], bf16)

        @pl.when(odd)
        def _():
            pair_copy().wait_recv()

        def step(k, _):
            @pl.when(odd)
            def _():
                @pl.when(z >= 3)
                def _():
                    to_odd(k).wait_recv()

                before = jnp.where(z >= 3, c_in[piece(k), :].astype(f32), 0.0) + pair_in[piece(k), :].astype(f32)
                c_out[piece(k), :] = (before + st[piece(k), :].astype(f32)).astype(bf16)
                sx[f, piece(k), :] = before.astype(bf16)

                @pl.when(z < last - 1)
                def _():
                    to_odd(k).start()

                @pl.when(z < last)
                def _():
                    to_even(k).start()

            @pl.when(jnp.logical_not(odd) & (z >= 2))
            def _():
                to_even(k).wait_recv()

            for n, target in enumerate((near[0], near[1], partner)):
                s_piece(n, k, f, target).start()
            return 0

        lax.fori_loop(0, CHUNKS, step, 0)

    @pl.when(chained)
    def _():
        @pl.when(z > HEAD)
        def _():
            pl.semaphore_wait(ready_sem, CHUNKS)
            chunks_out()

        chain()

        @pl.when(z == HEAD)
        def _():
            pl.semaphore_wait(ready_sem, CHUNKS)
            st[...] = c_out[...]
            chunks_out()

    def back(c):
        return remote(p2.at[c], sx.at[f, my_rows], p2_send.at[c], p2_recv.at[my_chunk], {"seq": c})

    def own_chunk():
        total = jnp.zeros((CHUNK, 2 * DV), f32)
        for c in range(HEAD + 1, n_seq):
            @pl.when(z != c - 1)
            def _():
                remote(
                    st.at[pl.ds(0, CHUNK)], p1.at[c - 1], p1_send.at[0], p1_recv.at[c - 1], {"seq": c - 1}
                ).wait_recv()

            total = total + p1[c - 1].astype(f32)
            if c >= CHAIN:
                p2[c] = total.astype(bf16)

                @pl.when(z != c)
                def _():
                    back(c).start()

        sx[f, my_rows, :] = p2[z]

    def from_owners():
        def step(k, _):
            @pl.when(z != FIRST_OWNER + k)
            def _():
                remote(
                    p2.at[0], sx.at[f, piece(k)], p2_send.at[0], p2_recv.at[k], {"feat": partner}
                ).wait_recv()

            for n, target in enumerate((near[0], near[1], partner)):
                s_piece(n, k, f, target).start()
            return 0

        lax.fori_loop(0, CHUNKS, step, 0)

    def l_wait(source, b):
        remote(
            lown.at[pl.ds(0, rb)], lx.at[source, pl.ds(b * rb, rb)], l_send.at[0, 0],
            l_recv.at[source, b], {"feat": partner},
        ).wait_recv()

    relays = []
    onward = ((2 * yl, yr), (2 * yr + 1, yl))
    for k, (source, to) in enumerate(onward):
        q_copy(0, 0, source, partner).wait_recv()
        copy = remote(
            qx.at[source, pl.ds(0, 2 * DK)], qx.at[source, pl.ds(0, 2 * DK)],
            q_send.at[5 + k], q_recv.at[source], {"feat": 2 * to + core},
        )
        copy.start()
        relays.append(copy)

    def l_onward(k, b):
        source, to = onward[k]
        span = pl.ds(b * rb, rb)
        return remote(
            lx.at[source, span], lx.at[source, span], l_relay.at[k, b], l_recv.at[source, b],
            {"feat": 2 * to + core},
        )

    def relay(b):
        for k, (source, to) in enumerate(onward):
            l_wait(source, b)
            l_onward(k, b).start()

    def phi_of(source):
        @pl.when((source != 2 * yl) & (source != 2 * yr + 1))
        def _():
            q_copy(0, 0, source, partner).wait_recv()

        make_phi(source)

    def phi_near(g, _):
        phi_of(jnp.where(g < 4, 2 * jnp.where(g < 2, yr, yl) + g % 2, partner))
        return 0

    def phi_far(g, _):
        phi_of(2 * yo + g)
        return 0

    @pl.when(jnp.logical_not(chained))
    def _():
        lax.fori_loop(0, 5, phi_near, 0)

    relay(0)

    @pl.when(owns)
    def _():
        own_chunk()

    relay(1)

    @pl.when(chained)
    def _():
        lax.fori_loop(0, 5, phi_near, 0)

    @pl.when(jnp.logical_not(chained))
    def _():
        from_owners()


    def s_wait(source):
        for k in range(CHUNKS):
            s_piece(0, k, source, partner).wait_recv()

    def s_pass(n):
        for k in range(CHUNKS):
            s_piece(0, k, near[n], partner).wait_recv()
            if n < 2:
                @pl.when(core == 1 - n)
                def _():
                    s_piece(6, k, near[n], near[1 - n]).start()
            s_piece(3 + n, k, near[n], partner).start()

    lax.fori_loop(0, 2, phi_far, 0)
    w_copy.wait_recv()

    def finish(units, first=False):
        for u, (source, b) in enumerate(units):
            span = pl.ds(b * rb, rb)
            for h in range(2):
                lanes = pl.ds(h * DV, DV)
                number = jnp.dot(
                    phi[source, h, span, :], sx[source, :, lanes], preferred_element_type=f32
                ) + lx[source, span, lanes].astype(f32)
                scale = lax.rsqrt(jnp.mean(number * number, axis=-1, keepdims=True) + 4e-6)
                nrm[u, :, lanes] = (number * scale).astype(bf16)
        for b in range(2):
            span = pl.ds(b * rb, rb)
            mine = [(u, source) for u, (source, bb) in enumerate(units) if bb == b]
            for k, which in enumerate((other, core)):
                if mine:
                    term = sum(
                        jnp.dot(
                            nrm[u], wo_v[which, pl.ds(pl.multiple_of(source * 2 * DV, 2 * DV), 2 * DV), :],
                            preferred_element_type=f32,
                        )
                        for u, source in mine
                    )
                    acc[k, span, :] = term if first else acc[k, span, :] + term

    def l_wait_unless_relayed(source, b):
        @pl.when((source != 2 * yl) & (source != 2 * yr + 1))
        def _():
            l_wait(source, b)

    finish([(f, 0), (f, 1)], first=True)
    s_wait(partner)
    for b in range(2):
        l_wait(partner, b)
    finish([(partner, 0), (partner, 1)])
    def sides(sources):
        units = [(source, b) for source in sources for b in range(2)]
        for source, b in units:
            l_wait_unless_relayed(source, b)
        finish(units)

    s_pass(0)
    s_pass(1)
    sides(near[:2])
    s_pass(2)
    s_wait(beyond[0])
    s_wait(beyond[1])
    sides(beyond[:2])
    s_wait(beyond[2])
    out_copies = []
    for b in range(2):
        units = [(near[2], b), (beyond[2], b)]
        for source, _ in units:
            l_wait(source, b)
        finish(units)
        span = pl.ds(b * rb, rb)
        mine = pl.ds(pl.multiple_of(core * half + b * rb, rb), rb)
        outp[span, :] = acc[0, span, :].astype(bf16)
        out_copy = remote(outp.at[span], out.at[mine], o_send.at[b], o_recv.at[b], {"feat": partner})
        out_copy.start()
        out_copies.append(out_copy)
        out[mine, :] = acc[1, span, :].astype(bf16)

    with jax.named_scope('tail_sends'):
        @pl.when(chained & jnp.logical_not(odd))
        def _():
            pair_copy().wait_send()

        for k in range(CHUNKS):
            @pl.when(chained & odd & (z < last - 1))
            def _():
                to_odd(k).wait_send()

            @pl.when(chained & odd & (z < last))
            def _():
                to_even(k).wait_send()

            @pl.when(gives & (z != FIRST_OWNER + k))
            def _():
                to_owner(k).wait_send()

        @pl.when(owns)
        def _():
            for c in range(CHAIN, n_seq):
                @pl.when(z != c)
                def _():
                    back(c).wait_send()

        for r in range(4):
            @pl.when(core != r // 2)
            def _():
                across(r).wait_send()

        for copy in l_copies + q_copies + [w_copy] + relays + out_copies:
            copy.wait_send()
        for k in range(2):
            for b in range(2):
                l_onward(k, b).wait_send()
        for n, source in enumerate((f, f, f, near[0], near[1], near[2], f)):
            for k in range(CHUNKS):
                s_piece(n, k, source, partner).wait_send()
    with jax.named_scope('tail_recv'):
        for b in range(2):
            theirs = pl.ds(pl.multiple_of(other * half + b * rb, rb), rb)
            remote(
                outp.at[pl.ds(b * rb, rb)], out.at[theirs], o_send.at[b], o_recv.at[b], {"feat": partner}
            ).wait_recv()


def local(n_seq, consts, tokens, w_query, w_key, value_weight, w_out):
    rows, deep = tokens.shape
    cols = value_weight.shape[1]
    half = rows // 2
    f32, bf16 = jnp.float32, jnp.bfloat16
    dma = pltpu.SemaphoreType.DMA
    anywhere = pl.BlockSpec(memory_space=pl.ANY)
    vm = pltpu.VMEM
    width = w_query.shape[1]
    mixed = pl.pallas_call(
        functools.partial(kernel, n_seq),
        out_shape=pltpu.VMEM((rows, cols), bf16),
        in_specs=[anywhere] * 9,
        out_specs=pl.BlockSpec(memory_space=pltpu.VMEM),
        scratch_shapes=[
            vm((rows, deep), bf16), vm((width, deep), bf16), vm((width, deep), bf16),
            vm((deep, cols), bf16), vm((deep, LANES), bf16), vm((2, 8 * cols, cols), bf16),
            vm((2 * FEATS, LANES), bf16), vm((2 * FEATS, LANES), bf16),
            vm((2 * FEATS, 3 * DK), bf16), vm((2 * FEATS, 3 * DK), bf16),
            vm((rows, LANES), bf16), vm((LANES, rows), bf16), vm((2, LANES, rows), bf16),
            vm((rows, cols), bf16), vm((FEATS, cols), f32), vm((FEATS, cols), bf16),
            vm((n_seq, CHUNK, cols), bf16), vm((n_seq, CHUNK, cols), bf16),
            vm((FEATS, cols), bf16), vm((FEATS, cols), bf16), vm((FEATS, cols), bf16),
            vm((8, 3 * DK, half), bf16), vm((8, 2, half, FEATS), bf16), vm((8, FEATS, cols), bf16),
            vm((rows, cols), bf16), vm((8, half, cols), bf16),
            vm((4, half // 2, cols), bf16), vm((2, half, cols), f32), vm((half, cols), bf16),
            dma((12,)), pltpu.SemaphoreType.REGULAR,
            dma((CHUNKS,)), dma((n_seq,)), dma((n_seq,)), dma((CHUNKS,)), dma, dma, dma((2, CHUNKS)), dma((CHUNKS,)), dma((CHUNKS,)),
            dma((7,)), dma((8,)), dma, dma,
            dma((4, 3)), dma((2, 2)), dma((8, 2)), dma((7, CHUNKS)), dma((8, CHUNKS)), dma((2,)), dma((2,)),
        ],
        compiler_params=pltpu.CompilerParams(
            collective_id=0, has_side_effects=True, vmem_limit_bytes=56 * 1024 * 1024
        ),
    )(tokens, w_query.T, w_key.T, value_weight, w_out, *consts)
    return mixed


def solution(mesh):
    consts = [
        jnp.asarray(e, jnp.bfloat16)
        for e in (*selectors(2 * DK, ONE, LANES, False), *selectors(0, 2 * DK, 3 * DK, True))
    ]
    placed = (P(("dp", "seq"), None),) + (P(None, "feat"),) * 4

    def run(*args):
        return jax.shard_map(
            functools.partial(local, mesh.shape["seq"], consts),
            mesh=mesh, in_specs=placed, out_specs=P(("dp", "seq"), "feat"), check_vma=False,
        )(*args)

    return run
```
